32 devices in a mesh: blk: 16 (over z, x, core), col: 2 (over y).
Axes of the slice: x: 2, y: 2, z: 4, core: 2. Of those that a mesh axis runs over, the one named last changes fastest.
Arguments:
- blocks: bfloat16 [16, 2, 2048, 2048], P('blk'), may hold values from -0.09375 to 0.09375
- offsets: int32 [16, 2], P('blk'), may hold values from -2 to 2, as said below
- krylov: bfloat16 [16, 64, 32768], P('col', None, 'blk'), may hold values from -6 to 6
- previous: float32 [64, 16, 32768], P(None, 'col', 'blk')
- node_table: float32 [32], replicated, may hold values from -1.5 to 1.5
- node_index: int32 [16], P('col'), may hold values from 0 to 31
- pole_values: float32 [16], P('col'), may hold values from 4 to 16
- scaling: float32 [16], P('col'), may hold values from 0.5 to 2
Outputs:
- new_basis: bfloat16 [16, 64, 32768], P('col', None, 'blk')
- first_coeffs: float32 [64, 64], replicated
- second_coeffs: float32 [64, 64], replicated
- factor: float32 [64, 64], replicated
The draws below stay inside these ranges and needn't reach their ends.
Inputs may be any that keep to these rules, and one draw needn't show every extreme that they name: `offsets`: each block row's 2 distances are distinct.
All inputs are finite; a program needn't handle non-finite values.
Results may differ from the reference program's by a relative error of at most 0.0012.
Values may be sent and summed in bfloat16 or wider, within the bound.
A program may use at most 128 MiB of HBM per device.

```python
import math
import jax
import jax.numpy as jnp
from jax import lax

BLOCK_ROWS = 2048
KRYLOV_COLS = 64
TERMS = 16
COUPLINGS = 2
REACH = 2
NODE_COUNT = 32
PREV_COLS = 64
ROWS = 32768
N_BLK = 16


def draw_offsets(key, part):
    width = 2 * REACH + 1
    scores = jax.random.randint(key, (N_BLK, width), 0, 1 << 20) * width + jnp.arange(width, dtype=jnp.int32)[None, :]
    chosen = lax.top_k(scores, COUPLINGS)[1]
    return (chosen - REACH).astype(jnp.int32)


def draw_previous(key, part):
    own_key = jax.random.fold_in(key, 11)
    common_key = jax.random.fold_in(key, 12)
    own = jax.random.normal(own_key, (PREV_COLS, TERMS, ROWS), jnp.float32)
    common = jax.random.normal(common_key, (1, TERMS, ROWS), jnp.float32)
    return (own + 0.125 * common).astype(jnp.float32)


def place_ends(array, stream_key, least, high):
    spot = [jax.random.randint(jax.random.fold_in(stream_key, axis), (), 0, length) for axis, length in enumerate(array.shape)]
    longest = array.shape.index(max(array.shape))
    next_to = spot[:longest] + [(spot[longest] + 1) % array.shape[longest]] + spot[longest + 1:]
    return array.at[tuple(spot)].set(least).at[tuple(next_to)].set(high)


def block_levels(rng, extent, split, low, high):
    factor_of = 1.0
    for axis_at, blocks in split:
        draws = jax.random.uniform(jax.random.fold_in(jax.random.fold_in(rng, 6), axis_at), (blocks,), jnp.float32, low / len(split), high / len(split))
        factor_of = factor_of * jnp.repeat(jnp.exp(draws), extent[axis_at] // blocks).reshape((-1,) + (1,) * (len(extent) - 1 - axis_at))
    return factor_of


def gaussian(rng, shape, scale, reach, cuts=(), kind=jnp.bfloat16):
    entries = scale * jax.random.normal(rng, shape, jnp.float32)
    if cuts:
        entries = entries * block_levels(rng, shape, cuts, -0.22, 0.18)
    return jnp.clip(entries, -reach, reach).astype(kind)


def setup_inputs(seed: int = 0) -> dict:
    arg_keys = jax.random.split(jax.random.key(seed), 9)
    blocks = gaussian(arg_keys[0], (N_BLK, COUPLINGS, BLOCK_ROWS, BLOCK_ROWS), (COUPLINGS * BLOCK_ROWS) ** -0.5, 0.09375, ((0, 16),))
    offsets = draw_offsets(jax.random.fold_in(arg_keys[8], 71), 0)
    krylov = gaussian(arg_keys[2], (TERMS, KRYLOV_COLS, ROWS), 1.0, 6.0, ((0, 2), (2, 16)))
    previous = draw_previous(jax.random.fold_in(arg_keys[8], 71), 0)
    node_table = jnp.clip(jax.random.uniform(arg_keys[4], (NODE_COUNT,), jnp.float32, -1.5, 1.5), -1.5, 1.5)
    node_index = place_ends(jax.random.randint(arg_keys[5], (TERMS,), 0, NODE_COUNT), jax.random.fold_in(arg_keys[5], 1), 0, NODE_COUNT - 1).astype(jnp.int32)
    pole_values = jnp.clip(jnp.exp(math.log(16.0) - 1.3862944 * jax.random.uniform(arg_keys[6], (TERMS,), jnp.float32) ** block_levels(arg_keys[6], (TERMS,), ((0, 2),), -0.2, 0.2)), 4.0, 16.0)
    scaling = jnp.clip(jnp.exp(math.log(2.0) - 1.3862944 * jax.random.uniform(arg_keys[7], (TERMS,), jnp.float32) ** block_levels(arg_keys[7], (TERMS,), ((0, 2),), -0.2, 0.2)), 0.5, 2.0)
    return {"blocks": blocks, "offsets": offsets, "krylov": krylov, "previous": previous, "node_table": node_table, "node_index": node_index, "pole_values": pole_values, "scaling": scaling}


exact_mode = lax.Precision.HIGHEST

def apply_band(blocks, offsets, krylov):
    flat = krylov.reshape(TERMS * KRYLOV_COLS, N_BLK, BLOCK_ROWS)

    def one_row(item):
        position, band, distances = item
        total = jnp.zeros((TERMS * KRYLOV_COLS, BLOCK_ROWS), jnp.float32)
        for coupling in range(COUPLINGS):
            source = ((position + distances[coupling]) % N_BLK).astype(jnp.int32)
            piece = lax.dynamic_index_in_dim(flat, source, 1, keepdims=False)
            total = total + lax.dot_general(piece.astype(jnp.float32), band[coupling].astype(jnp.float32), (((1,), (1,)), ((), ())), preferred_element_type=jnp.float32)
        return total
    image = lax.map(one_row, (jnp.arange(N_BLK, dtype=jnp.int32), blocks, offsets))
    return jnp.transpose(image, (1, 0, 2)).reshape(TERMS, KRYLOV_COLS, N_BLK * BLOCK_ROWS)

def reference(blocks, offsets, krylov, previous, node_table, node_index, pole_values, scaling):
    image = apply_band(blocks, offsets, krylov)
    matches = node_index[:, None] == jnp.arange(NODE_COUNT, dtype=jnp.int32)[None, :]
    shift_value = lax.optimization_barrier(jnp.sum(jnp.where(matches, node_table[None, :], jnp.float32(0.0)), axis=1))
    carry_weight = scaling / (1.0 - shift_value / pole_values)
    before = jnp.concatenate([jnp.zeros_like(krylov[:1]), krylov[:-1]], axis=0)
    work = image - shift_value[:, None, None] * krylov.astype(jnp.float32) + carry_weight[:, None, None] * before.astype(jnp.float32)
    inverse_size = 1.0 / (ROWS * TERMS)
    root_size = math.sqrt(ROWS * TERMS)
    coeff_one = jnp.einsum('ptn,tmn->pm', previous, work, precision=exact_mode) * inverse_size
    first_pass = work - jnp.einsum('ptn,pm->tmn', previous, coeff_one, precision=exact_mode)
    coeff_two = jnp.einsum('ptn,tmn->pm', previous, first_pass, precision=exact_mode) * inverse_size
    second_pass = first_pass - jnp.einsum('ptn,pm->tmn', previous, coeff_two, precision=exact_mode)
    gram = jnp.einsum('tkn,tmn->km', second_pass, second_pass, precision=exact_mode) * inverse_size
    factor = jnp.linalg.cholesky(gram)
    identity = jnp.eye(KRYLOV_COLS, dtype=jnp.float32)
    inverse_factor = jax.scipy.linalg.solve_triangular(factor, identity, lower=True)
    new_basis = jnp.einsum('tkn,mk->tmn', second_pass, inverse_factor, precision=exact_mode).astype(jnp.bfloat16)
    return (new_basis, coeff_one * root_size, coeff_two * root_size, factor)
```

```python
import functools
import math

import jax
import jax.numpy as jnp
from jax import lax
from jax.experimental import pallas as pl
from jax.experimental.pallas import tpu as pltpu
from jax.sharding import PartitionSpec as P

REACH = 2
WIDTH = 2 * REACH + 1
PAIR = 2
CHUNK = 256
WINDOW = 3
LAG = 4
SENDS = 4
A_RING = 2 * WINDOW
B_SENDS = 6
D_RING = 2 * LAG + 2
BF = jnp.bfloat16
F32 = jnp.float32
NT = (((1,), (1,)), ((), ()))
MESH = pl.DeviceIdType.MESH


def split(x):
    high = x.astype(BF)
    return high, (x - high.astype(F32)).astype(BF)


def dot_nt(a, b):
    return lax.dot_general(a, b, NT, preferred_element_type=F32)


def exact(a, b):
    return jnp.dot(a, b, precision=lax.Precision.HIGHEST, preferred_element_type=F32)


def expand_kernel(
    n_blk, n_col, terms, cols, rows, total_size,
    offsets_in, node_index_in, node_table_in, pole_values_in, scaling_in,
    krylov, blocks, previous,
    wst, pst, reduced,
    offsets, node_index, node_table, pole_values, scaling, scalar_sem,
    bufs, carry, band, prev, image, sums, basis_sum,
    a_send, a_recv, b_send, b_recv, c_send, c_recv, d_send, d_recv,
    y_send, y_recv, own_sem, band_sem, prev_sem,
    part, rs_buf, z_buf, ag_buf, red_send, rs_recv, z_recv, ag_recv,
):
    me = lax.axis_index("blk")
    col = lax.axis_index("col")
    core = lax.rem(me, 2)
    chip = lax.div(me, 2)
    par = lax.rem(chip, 2)
    n_chip = n_blk // 2
    n_prev = previous.shape[0]
    partner = (chip + 1 - 2 * par) * 2 + core
    ahead = lax.rem(chip + 2 - 4 * par + n_chip, n_chip) * 2 + core
    sibling = chip * 2 + 1 - core
    per_group = rows // CHUNK
    n_group = terms // PAIR
    n_piece = n_group * per_group

    def remote(src, dst, send, recv, blk, colpos=None):
        return pltpu.make_async_remote_copy(
            src_ref=src, dst_ref=dst, send_sem=send, recv_sem=recv,
            device_id=(blk, col if colpos is None else colpos), device_id_type=MESH)

    def place_of(s):
        if isinstance(s, int):
            return s // per_group, s % per_group
        return lax.div(s, per_group), lax.rem(s, per_group)

    def cut(s):
        group, k = place_of(s)
        return pl.ds(group * PAIR, PAIR), slice(None), pl.ds(pl.multiple_of(k * CHUNK, CHUNK), CHUNK)

    def ring(s, size):
        return s % size if isinstance(s, int) else lax.rem(s, size)

    def when(test, act):
        if isinstance(test, bool):
            if test:
                act()
        else:
            pl.when(test)(act)

    def a_copy(s):
        return remote(krylov.at[cut(s)], bufs.at[(4 * par,) + cut(s)], a_send.at[ring(s, SENDS)], a_recv.at[ring(s, A_RING)], partner)

    def b_copy(s):
        return remote(bufs.at[(4 - 4 * par,) + cut(s)], bufs.at[(4 * par,) + cut(s)], b_send.at[ring(s, B_SENDS)], b_recv.at[s], ahead)

    def d_copy(s):
        return remote(bufs.at[(4 - 4 * core,) + cut(s)], bufs.at[(3 - 2 * core,) + cut(s)], d_send.at[ring(s, SENDS)], d_recv.at[ring(s, D_RING)], sibling)

    c_copy = remote(krylov, bufs.at[1 + 2 * core], c_send, c_recv, sibling)
    own_copy = pltpu.make_async_copy(krylov, bufs.at[REACH], own_sem)
    band_copy = [pltpu.make_async_copy(blocks.at[0, c], band.at[c], band_sem.at[c]) for c in range(band.shape[0])]
    prev_copy = pltpu.make_async_copy(previous, prev, prev_sem)
    y_copy = remote(krylov.at[terms - 1], carry, y_send, y_recv, me, lax.rem(col + 1, n_col))

    team, depth = part.shape[0], z_buf.shape[0]
    place = lax.rem(me, 4)
    layer = lax.div(me, 4)
    pos = place * n_col + col

    def member(j):
        other = lax.rem(pos + j, team)
        return other, layer * 4 + lax.div(other, n_col), lax.rem(other, n_col)

    def peer(j):
        return lax.rem(layer + j, depth) * 4 + place

    def spread(src_of, dst_of, recv, targets):
        return [
            remote(src_of(j), dst_of(j), red_send.at[j - 1], recv.at[j - 1], *target)
            for j, target in targets]

    mates = [(j, member(j)[1:]) for j in range(1, team)]
    peers = [(j, (peer(j), col)) for j in range(1, depth)]
    rs_copy = spread(lambda j: part.at[member(j)[0]], lambda j: rs_buf.at[j - 1], rs_recv, mates)
    z_copy = spread(lambda j: z_buf.at[layer], lambda j: z_buf.at[layer], z_recv, peers)
    ag_copy = spread(lambda j: ag_buf.at[pos], lambda j: ag_buf.at[pos], ag_recv, mates)

    scalar_copy = [
        pltpu.make_async_copy(src, dst, scalar_sem.at[i])
        for i, (src, dst) in enumerate((
            (offsets_in, offsets), (node_index_in, node_index), (node_table_in, node_table),
            (pole_values_in, pole_values), (scaling_in, scaling)))]
    prev_copy.start()
    for copy in scalar_copy:
        copy.start()
    own_copy.start()
    for copy in band_copy:
        copy.start()

    barrier = pltpu.get_barrier_semaphore()
    for j in range(1, team):
        _, blk, at_col = member(j)
        pl.semaphore_signal(barrier, inc=1, device_id=(blk, at_col), device_id_type=MESH)
    for j in range(1, depth):
        pl.semaphore_signal(barrier, inc=1, device_id=(peer(j), col), device_id_type=MESH)
    pl.semaphore_wait(barrier, team + depth - 2)

    lax.fori_loop(0, WINDOW, lambda s, _: (a_copy(s).start(), 0)[1], 0)
    if n_col > 1:
        @pl.when(col < n_col - 1)
        def _():
            y_copy.start()
    c_copy.start()

    @pl.when(col == 0)
    def _():
        carry[...] = jnp.zeros_like(carry)

    lane = 256

    def arrange(t):
        p_at = t * 16

        def step(i, _):
            at = pl.ds(pl.multiple_of(i * lane, lane), lane)
            high, low = split(jnp.swapaxes(prev[p_at:p_at + 16, :, at], 0, 1))
            pst[:, p_at:p_at + 16, at] = high
            pst[:, n_prev + p_at:n_prev + p_at + 16, at] = low
            return 0
        lax.fori_loop(0, rows // lane, step, 0)

    def basis_term(t):
        part = dot_nt(pst[t], pst[t, :n_prev])
        if t == 0:
            basis_sum[...] = part
        else:
            basis_sum[...] += part

    def local_part(t):
        shift = jnp.full((8, 128), node_table[node_index[t]], F32)
        weight = jnp.full((8, 128), scaling[t], F32) / (
            1.0 - shift / jnp.full((8, 128), pole_values[t], F32))
        if t == 0 and n_col > 1:
            @pl.when(col > 0)
            def _():
                y_copy.wait_recv()
        before = carry[...] if t == 0 else bufs[REACH, t - 1]
        image[t * cols:(t + 1) * cols, :] = (
            weight[:1, :1] * before.astype(F32) - shift[:1, :1] * bufs[REACH, t].astype(F32))

    tile = 256
    n_coupling = band.shape[0]

    def selected(r):
        some, _, k_at = cut(r)
        slots = [bufs[j, some, :, k_at].reshape(PAIR * cols, CHUNK) for j in range(WIDTH)]
        picks = []
        for c in range(n_coupling):
            pick = slots[0]
            for j in range(1, WIDTH):
                pick = jnp.where(offsets[0, c] == j - REACH, slots[j], pick)
            picks.append(pick)
        return jnp.concatenate(picks, axis=1)

    def compute(r):
        group, k = place_of(r)
        k_at = pl.ds(pl.multiple_of(k * CHUNK, CHUNK), CHUNK)
        r_at = pl.ds(pl.multiple_of(group * PAIR * cols, PAIR * cols), PAIR * cols)
        left = selected(r)

        def step(i, _):
            at = pl.ds(pl.multiple_of(i * tile, tile), tile)
            right = jnp.concatenate([band[c, at, k_at] for c in range(n_coupling)], axis=1)
            image[r_at, at] += dot_nt(left, right)
            return 0
        lax.fori_loop(0, rows // tile, step, 0, unroll=UNROLL)

    def finish(t, first=False):
        at = pl.ds(t * cols, cols) if isinstance(t, int) else pl.ds(pl.multiple_of(t * cols, cols), cols)
        high, low = split(image[at, :])
        wst[t, :cols] = high
        wst[t, cols:] = low
        sums[...] += dot_nt(jnp.concatenate([pst[t], wst[t]], axis=0), wst[t])

    def ending():
        left = selected(n_piece - 1)
        k_at = pl.ds(rows - CHUNK, CHUNK)
        first = terms - PAIR
        acc = sums[...]
        for i in range(rows // tile):
            at = pl.ds(i * tile, tile)
            right = jnp.concatenate([band[c, at, k_at] for c in range(n_coupling)], axis=1)
            total = image[first * cols:, at] + dot_nt(left, right)
            for j in range(PAIR):
                t = first + j
                high, low = split(total[j * cols:(j + 1) * cols])
                wst[t, :cols, at] = high
                wst[t, cols:, at] = low
                both = jnp.concatenate([high, low], axis=0)
                acc = acc + dot_nt(jnp.concatenate([pst[t, :, at], both], axis=0), both)
        sums[...] = acc

    def forward_a(s):
        a_copy(s).wait_recv()
        when(s >= B_SENDS, lambda: b_copy(s - B_SENDS).wait_send())
        b_copy(s).start()

        @pl.when(par == core)
        def _():
            when(s >= SENDS, lambda: d_copy(s - SENDS).wait_send())
            d_copy(s).start()
        when(s + WINDOW >= SENDS, lambda: a_copy(s + WINDOW - SENDS).wait_send())
        when(s + WINDOW < n_piece, lambda: a_copy(s + WINDOW).start())

    def forward_b(s):
        b_copy(s).wait_recv()

        @pl.when(par != core)
        def _():
            when(s >= SENDS, lambda: d_copy(s - SENDS).wait_send())
            d_copy(s).start()

    def work_on(r):
        d_copy(r).wait_recv()
        compute(r)

    sums[...] = jnp.zeros_like(sums)
    prev_copy.wait()
    for t in range(n_prev // 16):
        arrange(t)
    for copy in scalar_copy:
        copy.wait()
    own_copy.wait()
    plan = {}
    for t in range(terms):
        plan.setdefault(t // 2, []).append(functools.partial(basis_term, t))
        plan.setdefault(t // 2, []).append(functools.partial(local_part, terms - 1 - t))
    for s in range(LAG + 1):
        forward_a(s)
        for item in plan.get(s, ()):
            item()
        if s >= LAG:
            forward_b(s - LAG)

    c_copy.wait_recv()
    for copy in band_copy:
        copy.wait()

    def main(s, _):
        forward_a(s)
        forward_b(s - LAG)
        r = s - LAG - 1
        work_on(r)
        group, k = place_of(r)

        @pl.when(k == per_group - 1)
        def _():
            for j in range(PAIR):
                finish(group * PAIR + j)
        return 0
    lax.fori_loop(LAG + 1, n_piece, main, 0)
    for s in range(n_piece, n_piece + LAG):
        forward_b(s - LAG)
        work_on(s - LAG - 1)
    d_copy(n_piece - 1).wait_recv()
    ending()
    total = sums[:n_prev] + sums[n_prev:2 * n_prev]
    gram = sums[2 * n_prev:2 * n_prev + cols] + sums[2 * n_prev + cols:]
    low = basis_sum[n_prev:]
    basis = basis_sum[:n_prev] + low + low.T
    full = jnp.concatenate([
        jnp.concatenate([total[:, :cols] + total[:, cols:], gram[:, :cols] + gram[:, cols:]], axis=1),
        jnp.concatenate([basis, jnp.zeros_like(basis)], axis=1)], axis=0)
    part[...] = full.reshape(part.shape)
    for copy in rs_copy:
        copy.start()
    total = part[pos]
    for j, copy in enumerate(rs_copy):
        copy.wait_recv()
        total = total + rs_buf[j]
    z_buf[layer] = total
    for copy in rs_copy:
        copy.wait_send()
    for copy in z_copy:
        copy.start()
    for s in range(n_piece - B_SENDS, n_piece):
        if s >= n_piece + WINDOW - SENDS:
            a_copy(s).wait_send()
        b_copy(s).wait_send()
        if s >= n_piece - SENDS:
            d_copy(s).wait_send()
    c_copy.wait_send()
    if n_col > 1:
        @pl.when(col < n_col - 1)
        def _():
            y_copy.wait_send()
    for copy in z_copy:
        copy.wait_recv()
    total = z_buf[0]
    for j in range(1, depth):
        total = total + z_buf[j]
    ag_buf[pos] = total
    for copy in z_copy:
        copy.wait_send()
    for copy in ag_copy:
        copy.start()
    for copy in ag_copy:
        copy.wait_recv()
    reduced[...] = ag_buf[...].reshape(reduced.shape)
    for copy in ag_copy:
        copy.wait_send()


UNROLL = 4


def expand(n_blk, n_col, blocks, offsets, krylov, previous, node_table, node_index, pole_values, scaling):
    terms, cols, rows = krylov.shape
    n_prev = previous.shape[0]
    hbm = pl.BlockSpec(memory_space=pl.ANY)
    vmem = pl.BlockSpec(memory_space=pltpu.VMEM)
    dma = pltpu.SemaphoreType.DMA
    team, depth = 4 * n_col, n_blk // 4
    n_piece = terms // PAIR * (rows // CHUNK)
    height = n_prev + cols
    piece = (height // team, 2 * cols)
    return pl.pallas_call(
        functools.partial(expand_kernel, n_blk, n_col, terms, cols, rows, rows * n_blk * terms * n_col),
        out_shape=(
            pltpu.VMEM((terms, 2 * cols, rows), BF),
            pltpu.VMEM((terms, 2 * n_prev, rows), BF),
            pltpu.VMEM((height, 2 * cols), F32),
        ),
        in_specs=[pl.BlockSpec(memory_space=pltpu.HBM)] * 5 + [hbm] * 3,
        out_specs=(vmem,) * 3,
        scratch_shapes=[
            pltpu.SMEM(x.shape, x.dtype) for x in (offsets, node_index, node_table, pole_values, scaling)
        ] + [
            dma((5,)),
            pltpu.VMEM((WIDTH, terms, cols, rows), BF),
            pltpu.VMEM((cols, rows), BF),
            pltpu.VMEM(blocks.shape[1:], BF),
            pltpu.VMEM(previous.shape, F32),
            pltpu.VMEM((terms * cols, rows), F32),
            pltpu.VMEM((2 * n_prev + 2 * cols, 2 * cols), F32),
            pltpu.VMEM((2 * n_prev, n_prev), F32),
        ] + [dma((n,)) for n in (SENDS, A_RING, B_SENDS, n_piece)] + [dma, dma] + [dma((n,)) for n in (SENDS, D_RING)]
        + [dma, dma, dma, dma((blocks.shape[1],)), dma] + [
            pltpu.VMEM((team,) + piece, F32),
            pltpu.VMEM((team - 1,) + piece, F32),
            pltpu.VMEM((depth,) + piece, F32),
            pltpu.VMEM((team,) + piece, F32),
        ] + [dma((n - 1,)) for n in (max(team, depth), team, depth, team)],
        compiler_params=pltpu.CompilerParams(
            collective_id=0, has_side_effects=True, vmem_limit_bytes=58589184),
    )(offsets, node_index, node_table, pole_values, scaling, krylov, blocks, previous)


def eliminate(both, cols):
    below = lax.broadcasted_iota(jnp.int32, (cols, 1), 0)
    k = 0
    while k < cols:
        width = 4 if k < 3 * cols // 8 else 8
        top = k // 8 * 8
        done, rest = both[:top], both[top:]
        row_at = below[top:]
        panel = [jnp.broadcast_to(rest[:, j:j + 1], rest.shape) for j in range(k, k + width)]
        for i in range(width):
            at = k + i - top
            ratio = jnp.where(row_at > k + i, panel[i] * (1.0 / panel[i][at:at + 1]), 0.0)
            for j in range(i + 1, width):
                panel[j] = panel[j] - ratio * panel[j][at:at + 1]
            rest = rest - ratio * rest[at:at + 1]
        both = jnp.concatenate([done, rest], axis=0) if top else rest
        k += width
    return both


def final_kernel(total_size, reduced, wst, pst, out, first_out, second_out, factor_out, first, second, factor, result, out_sem, small_sem):
    terms, depth, rows = wst.shape
    cols = depth // 2
    n_prev = first.shape[0]
    inverse_size = 1.0 / total_size
    root_size = math.sqrt(total_size)
    cross = reduced[:n_prev, :cols] * inverse_size
    self_gram = reduced[:n_prev, cols:] * inverse_size
    basis_gram = reduced[n_prev:, :n_prev] * inverse_size
    turned = cross.T
    once = exact(basis_gram, cross)
    coeff_two = cross - once
    combined = cross + coeff_two
    twice = exact(basis_gram, once)
    back = combined.T
    gram = self_gram - exact(
        jnp.concatenate([turned, back], axis=1),
        jnp.concatenate([combined, coeff_two - once + twice], axis=0))
    first[...] = cross * root_size
    second[...] = coeff_two * root_size
    small_copy = [
        pltpu.make_async_copy(src, dst, small_sem.at[i])
        for i, (src, dst) in enumerate(((first, first_out), (second, second_out), (factor, factor_out)))]
    small_copy[0].start()
    small_copy[1].start()
    row = lax.broadcasted_iota(jnp.int32, (cols, cols), 0)
    lane = lax.broadcasted_iota(jnp.int32, (cols, cols), 1)
    both = jnp.concatenate([gram, jnp.where(row == lane, 1.0, 0.0)], axis=1)
    both = eliminate(both, cols)
    left, right = both[:, :cols], both[:, cols:]
    pivots = jnp.sum(jnp.where(row == lane, left, 0.0), axis=1, keepdims=True)
    scale = 1.0 / jnp.sqrt(pivots)
    inverse = jnp.where(lane <= row, right * scale, 0.0)
    mix = -exact(inverse, back)
    fh, fl = split(inverse)
    dh, dl = split(mix)
    zero_f, zero_d = jnp.zeros_like(fl), jnp.zeros_like(dl)
    weights = jnp.concatenate([
        jnp.concatenate([fh, fh, dh, dh], axis=1),
        jnp.concatenate([fl, zero_f, dl, zero_d], axis=1),
    ], axis=0)
    factor[...] = jnp.where(lane >= row, left * scale, 0.0).T
    small_copy[2].start()
    out_copy = [pltpu.make_async_copy(result.at[t], out.at[t], out_sem.at[t]) for t in range(terms)]
    for t in range(terms):
        both = jnp.dot(weights, jnp.concatenate([wst[t], pst[t]], axis=0), preferred_element_type=F32)
        result[t] = (both[:cols] + both[cols:]).astype(BF)
        out_copy[t].start()
    for copy in small_copy + out_copy:
        copy.wait()


def final(total_size, reduced, wst, pst):
    terms, _, rows = wst.shape
    cols, n_prev = wst.shape[1] // 2, pst.shape[1] // 2
    vmem = pl.BlockSpec(memory_space=pltpu.VMEM)
    hbm = pl.BlockSpec(memory_space=pl.ANY)
    shape = jax.ShapeDtypeStruct
    dma = pltpu.SemaphoreType.DMA
    return pl.pallas_call(
        functools.partial(final_kernel, total_size),
        out_shape=(shape((terms, cols, rows), BF), shape((n_prev, cols), F32), shape((n_prev, cols), F32), shape((cols, cols), F32)),
        in_specs=[vmem] * 3,
        out_specs=(hbm,) * 4,
        scratch_shapes=[
            pltpu.VMEM((n_prev, cols), F32),
            pltpu.VMEM((n_prev, cols), F32),
            pltpu.VMEM((cols, cols), F32),
            pltpu.VMEM((terms, cols, rows), BF),
            dma((terms,)), dma((3,)),
        ],
        compiler_params=pltpu.CompilerParams(vmem_limit_bytes=20 * 1024 * 1024),
    )(reduced, wst, pst)


def body(n_blk, n_col, blocks, offsets, krylov, previous, node_table, node_index, pole_values, scaling):
    terms, cols, rows = krylov.shape
    wst, pst, reduced = expand(
        n_blk, n_col, blocks, offsets, krylov, previous, node_table, node_index, pole_values, scaling)
    return final(rows * n_blk * terms * n_col, reduced, wst, pst)


def solution(mesh):
    in_specs = (
        P("blk", None, None, None),
        P("blk", None),
        P("col", None, "blk"),
        P(None, "col", "blk"),
        P(),
        P("col"),
        P("col"),
        P("col"),
    )
    out_specs = (P("col", None, "blk"), P(), P(), P())
    call = functools.partial(body, mesh.shape["blk"], mesh.shape["col"])
    return jax.shard_map(call, mesh=mesh, in_specs=in_specs, out_specs=out_specs, check_vma=False)
```

```python
import functools
import math

import jax
import jax.numpy as jnp
from jax import lax
from jax.experimental import pallas as pl
from jax.experimental.pallas import tpu as pltpu
from jax.sharding import PartitionSpec as P

REACH = 2
WIDTH = 2 * REACH + 1
GROUP = 2
CHUNK = 256
WINDOW = 3
LAG = 4
SENDS = 4
A_RING = 2 * WINDOW
B_SENDS = 6
D_RING = LAG + 6
BF = jnp.bfloat16
F32 = jnp.float32
NT = (((1,), (1,)), ((), ()))
MESH = pl.DeviceIdType.MESH


def split(x):
    high = x.astype(BF)
    return high, (x - high.astype(F32)).astype(BF)


def dot_nt(a, b):
    return lax.dot_general(a, b, NT, preferred_element_type=F32)


def exact(a, b):
    return jnp.dot(a, b, precision=lax.Precision.HIGHEST, preferred_element_type=F32)


def expand_kernel(
    n_blk, n_col, terms, cols, rows, total_size,
    offsets_in, node_index_in, node_table_in, pole_values_in, scaling_in,
    krylov, blocks, previous,
    wst, pst, reduced,
    offsets, node_index, node_table, pole_values, scaling, scalar_sem,
    bufs, carry, band, prev, image, sums, basis_sum,
    a_send, a_recv, b_send, b_recv, c_send, c_recv, d_send, d_recv,
    y_send, y_recv, own_sem, band_sem, prev_sem,
    part, rs_buf, z_buf, ag_buf, red_send, rs_recv, z_recv, ag_recv,
):
    me = lax.axis_index("blk")
    col = lax.axis_index("col")
    core = lax.rem(me, 2)
    chip = lax.div(me, 2)
    par = lax.rem(chip, 2)
    n_chip = n_blk // 2
    n_prev = previous.shape[0]
    partner = (chip + 1 - 2 * par) * 2 + core
    ahead = lax.rem(chip + 2 - 4 * par + n_chip, n_chip) * 2 + core
    sibling = chip * 2 + 1 - core
    per_group = rows // CHUNK
    n_group = terms // GROUP
    n_piece = n_group * per_group

    def remote(src, dst, send, recv, blk, colpos=None):
        return pltpu.make_async_remote_copy(
            src_ref=src, dst_ref=dst, send_sem=send, recv_sem=recv,
            device_id=(blk, col if colpos is None else colpos), device_id_type=MESH)

    def place_of(s):
        if isinstance(s, int):
            return s // per_group, s % per_group
        return lax.div(s, per_group), lax.rem(s, per_group)

    def cut(s):
        group, k = place_of(s)
        return pl.ds(group * GROUP, GROUP), slice(None), pl.ds(pl.multiple_of(k * CHUNK, CHUNK), CHUNK)

    def ring(s, size):
        return s % size if isinstance(s, int) else lax.rem(s, size)

    def when(test, act):
        if isinstance(test, bool):
            if test:
                act()
        else:
            pl.when(test)(act)

    def a_copy(s):
        return remote(bufs.at[(REACH,) + cut(s)], bufs.at[(4 * par,) + cut(s)], a_send.at[ring(s, SENDS)], a_recv.at[ring(s, A_RING)], partner)

    def b_copy(s):
        return remote(bufs.at[(4 - 4 * par,) + cut(s)], bufs.at[(4 * par,) + cut(s)], b_send.at[ring(s, B_SENDS)], b_recv.at[s], ahead)

    def d_copy(s):
        return remote(bufs.at[(4 - 4 * core,) + cut(s)], bufs.at[(3 - 2 * core,) + cut(s)], d_send.at[ring(s, SENDS)], d_recv.at[ring(s, D_RING)], sibling)

    c_copy = remote(krylov, bufs.at[1 + 2 * core], c_send, c_recv, sibling)
    own_copy = []
    for g in range(n_group):
        some = pl.ds(g * GROUP, GROUP)
        own_copy.append(pltpu.make_async_copy(krylov.at[some], bufs.at[REACH, some], own_sem.at[g]))
    band_copy = [pltpu.make_async_copy(blocks.at[0, c], band.at[c], band_sem.at[c]) for c in range(band.shape[0])]
    prev_copy = pltpu.make_async_copy(previous, prev, prev_sem)
    y_copy = remote(krylov.at[terms - 1], carry, y_send, y_recv, me, lax.rem(col + 1, n_col))

    team, depth = part.shape[0], z_buf.shape[0]
    half = team // 2
    place = lax.rem(me, 4)
    layer = lax.div(me, 4)
    pos = place * n_col + col

    def member(j):
        other = lax.rem(pos + j, team)
        return other, layer * 4 + lax.div(other, n_col), lax.rem(other, n_col)

    def peer(j):
        return lax.rem(layer + j, depth) * 4 + place

    def spread(src_of, dst_of, recv, targets):
        return [
            remote(src_of(j), dst_of(j), red_send.at[j - 1], recv.at[j - 1], *target)
            for j, target in targets]

    mates = [(j, member(j)[1:]) for j in range(1, team)]
    peers = [(j, (peer(j), col)) for j in range(1, depth)]
    rs_copy = spread(lambda j: part.at[member(j)[0]], lambda j: rs_buf.at[j - 1], rs_recv, mates)
    z_copy = spread(lambda j: z_buf.at[layer], lambda j: z_buf.at[layer], z_recv, peers)
    ag_copy = spread(lambda j: ag_buf.at[pos], lambda j: ag_buf.at[pos], ag_recv, mates)

    scalar_copy = [
        pltpu.make_async_copy(src, dst, scalar_sem.at[i])
        for i, (src, dst) in enumerate((
            (offsets_in, offsets), (node_index_in, node_index), (node_table_in, node_table),
            (pole_values_in, pole_values), (scaling_in, scaling)))]
    own_copy[0].start()
    for copy in scalar_copy:
        copy.start()
    prev_copy.start()
    for copy in own_copy[1:]:
        copy.start()

    barrier = pltpu.get_barrier_semaphore()
    for j in range(1, team):
        _, blk, at_col = member(j)
        pl.semaphore_signal(barrier, inc=1, device_id=(blk, at_col), device_id_type=MESH)
    for j in range(1, depth):
        pl.semaphore_signal(barrier, inc=1, device_id=(peer(j), col), device_id_type=MESH)
    pl.semaphore_wait(barrier, team + depth - 2)

    own_copy[0].wait()
    lax.fori_loop(0, WINDOW, lambda s, _: (a_copy(s).start(), 0)[1], 0)
    if n_col > 1:
        @pl.when(col < n_col - 1)
        def _():
            y_copy.start()
    c_copy.start()
    for copy in band_copy:
        copy.start()

    @pl.when(col == 0)
    def _():
        carry[...] = jnp.zeros_like(carry)

    lane = 256

    def arrange(t):
        p_at = t * 16

        def step(i, _):
            at = pl.ds(pl.multiple_of(i * lane, lane), lane)
            high, low = split(jnp.swapaxes(prev[p_at:p_at + 16, :, at], 0, 1))
            pst[:, p_at:p_at + 16, at] = high
            pst[:, n_prev + p_at:n_prev + p_at + 16, at] = low
            return 0
        lax.fori_loop(0, rows // lane, step, 0)

    def basis_term(t):
        part = dot_nt(pst[t], pst[t, :n_prev])
        if t == 0:
            basis_sum[...] = part
        else:
            basis_sum[...] += part

    def local_part(t):
        shift = jnp.full((8, 128), node_table[node_index[t]], F32)
        weight = jnp.full((8, 128), scaling[t], F32) / (
            1.0 - shift / jnp.full((8, 128), pole_values[t], F32))
        if t == 0 and n_col > 1:
            @pl.when(col > 0)
            def _():
                y_copy.wait_recv()
        before = carry[...] if t == 0 else bufs[REACH, t - 1]
        image[t * cols:(t + 1) * cols, :] = (
            weight[:1, :1] * before.astype(F32) - shift[:1, :1] * bufs[REACH, t].astype(F32))

    tile = 256
    n_coupling = band.shape[0]

    def selected(r):
        some, _, k_at = cut(r)
        slots = [bufs[j, some, :, k_at].reshape(GROUP * cols, k_at.size) for j in range(WIDTH)]
        picks = []
        for c in range(n_coupling):
            pick = slots[0]
            for j in range(1, WIDTH):
                pick = jnp.where(offsets[0, c] == j - REACH, slots[j], pick)
            picks.append(pick)
        return jnp.concatenate(picks, axis=1)

    def weights_at(at, k_at):
        return jnp.concatenate([band[c, at, k_at] for c in range(n_coupling)], axis=1)

    def compute(r):
        some, _, k_at = cut(r)
        first = some.start * cols
        r_at = pl.ds(first if isinstance(r, int) else pl.multiple_of(first, GROUP * cols), GROUP * cols)
        left = selected(r)

        def step(i, _):
            at = pl.ds(pl.multiple_of(i * tile, tile), tile)
            image[r_at, at] += dot_nt(left, weights_at(at, k_at))
            return 0
        lax.fori_loop(0, rows // tile, step, 0, unroll=UNROLL)

    def finish(t):
        at = pl.ds(t * cols, cols) if isinstance(t, int) else pl.ds(pl.multiple_of(t * cols, cols), cols)
        high, low = split(image[at, :])
        wst[t, :cols] = high
        wst[t, cols:] = low
        sums[...] += dot_nt(jnp.concatenate([pst[t], wst[t]], axis=0), wst[t])

    def forward_a(s):
        a_copy(s).wait_recv()
        when(s >= B_SENDS, lambda: b_copy(s - B_SENDS).wait_send())
        b_copy(s).start()

        @pl.when(par == core)
        def _():
            when(s >= SENDS, lambda: d_copy(s - SENDS).wait_send())
            d_copy(s).start()
        when(s + WINDOW >= SENDS, lambda: a_copy(s + WINDOW - SENDS).wait_send())
        when(s + WINDOW < n_piece, lambda: a_copy(s + WINDOW).start())

    def forward_b(s):
        b_copy(s).wait_recv()

        @pl.when(par != core)
        def _():
            when(s >= SENDS, lambda: d_copy(s - SENDS).wait_send())
            d_copy(s).start()

    def work_on(r):
        d_copy(r).wait_recv()
        compute(r)

    sums[...] = jnp.zeros_like(sums)
    prev_copy.wait()
    for t in range(n_prev // 16):
        arrange(t)
    for copy in scalar_copy + own_copy[1:]:
        copy.wait()
    plan = {}
    for t in range(terms):
        at = t * (LAG + 1) // terms
        plan.setdefault(at, []).append(functools.partial(basis_term, t))
        plan.setdefault(at, []).append(functools.partial(local_part, terms - 1 - t))
    for s in range(LAG + 1):
        forward_a(s)
        for item in plan.get(s, ()):
            item()
        if s >= LAG:
            forward_b(s - LAG)
    low = basis_sum[n_prev:]
    basis = basis_sum[:n_prev] + low + low.T
    part[half:] = jnp.concatenate([basis, jnp.zeros_like(basis)], axis=1).reshape(half, *part.shape[1:])
    c_copy.wait_recv()
    for copy in band_copy:
        copy.wait()

    def main(s, _):
        @pl.when(s < n_piece)
        def _():
            forward_a(s)
        r = s - LAG - 2
        @pl.when(r >= 0)
        def _():
            work_on(r)
        group, k = place_of(r)

        @pl.when((r >= 0) & (k == per_group - 1))
        def _():
            for j in range(GROUP):
                finish(group * GROUP + j)
        @pl.when(s < n_piece + LAG)
        def _():
            forward_b(s - LAG)
        return 0
    lax.fori_loop(LAG + 1, n_piece + LAG + 2, main, 0)
    total = sums[:n_prev] + sums[n_prev:2 * n_prev]
    gram = sums[2 * n_prev:2 * n_prev + cols] + sums[2 * n_prev + cols:]
    full = jnp.concatenate([total[:, :cols] + total[:, cols:], gram[:, :cols] + gram[:, cols:]], axis=1)
    part[:half] = full.reshape(half, *part.shape[1:])
    for copy in rs_copy:
        copy.start()
    total = part[pos]
    for j, copy in enumerate(rs_copy):
        copy.wait_recv()
        total = total + rs_buf[j]
    z_buf[layer] = total
    for copy in rs_copy:
        copy.wait_send()
    for copy in z_copy:
        copy.start()
    for s in range(n_piece - B_SENDS, n_piece):
        if s >= n_piece + WINDOW - SENDS:
            a_copy(s).wait_send()
        b_copy(s).wait_send()
        if s >= n_piece - SENDS:
            d_copy(s).wait_send()
    c_copy.wait_send()
    if n_col > 1:
        @pl.when(col < n_col - 1)
        def _():
            y_copy.wait_send()
    for copy in z_copy:
        copy.wait_recv()
    total = z_buf[0]
    for j in range(1, depth):
        total = total + z_buf[j]
    ag_buf[pos] = total
    for copy in z_copy:
        copy.wait_send()
    for copy in ag_copy:
        copy.start()
    for copy in ag_copy:
        copy.wait_recv()
    reduced[...] = ag_buf[...].reshape(reduced.shape)
    for copy in ag_copy:
        copy.wait_send()


UNROLL = 8


def expand(n_blk, n_col, blocks, offsets, krylov, previous, node_table, node_index, pole_values, scaling):
    terms, cols, rows = krylov.shape
    n_prev = previous.shape[0]
    hbm = pl.BlockSpec(memory_space=pl.ANY)
    vmem = pl.BlockSpec(memory_space=pltpu.VMEM)
    dma = pltpu.SemaphoreType.DMA
    team, depth = 4 * n_col, n_blk // 4
    n_group = terms // GROUP
    n_piece = n_group * (rows // CHUNK)
    height = n_prev + cols
    piece = (height // team, 2 * cols)
    return pl.pallas_call(
        functools.partial(expand_kernel, n_blk, n_col, terms, cols, rows, rows * n_blk * terms * n_col),
        out_shape=(
            pltpu.VMEM((terms, 2 * cols, rows), BF),
            pltpu.VMEM((terms, 2 * n_prev, rows), BF),
            pltpu.VMEM((height, 2 * cols), F32),
        ),
        in_specs=[pl.BlockSpec(memory_space=pltpu.HBM)] * 5 + [hbm] * 3,
        out_specs=(vmem,) * 3,
        scratch_shapes=[
            pltpu.SMEM(x.shape, x.dtype) for x in (offsets, node_index, node_table, pole_values, scaling)
        ] + [
            dma((5,)),
            pltpu.VMEM((WIDTH, terms, cols, rows), BF),
            pltpu.VMEM((cols, rows), BF),
            pltpu.VMEM(blocks.shape[1:], BF),
            pltpu.VMEM(previous.shape, F32),
            pltpu.VMEM((terms * cols, rows), F32),
            pltpu.VMEM((2 * n_prev + 2 * cols, 2 * cols), F32),
            pltpu.VMEM((2 * n_prev, n_prev), F32),
        ] + [dma((n,)) for n in (SENDS, A_RING, B_SENDS, n_piece)] + [dma, dma] + [dma((n,)) for n in (SENDS, D_RING)]
        + [dma, dma, dma((n_group,)), dma((blocks.shape[1],)), dma] + [
            pltpu.VMEM((team,) + piece, F32),
            pltpu.VMEM((team - 1,) + piece, F32),
            pltpu.VMEM((depth,) + piece, F32),
            pltpu.VMEM((team,) + piece, F32),
        ] + [dma((n - 1,)) for n in (max(team, depth), team, depth, team)],
        compiler_params=pltpu.CompilerParams(
            collective_id=0, has_side_effects=True, vmem_limit_bytes=58589184),
    )(offsets, node_index, node_table, pole_values, scaling, krylov, blocks, previous)


def eliminate(both, cols):
    below = lax.broadcasted_iota(jnp.int32, (cols, 1), 0)
    k = 0
    while k < cols:
        width = 4 if k < 3 * cols // 8 else 8
        top = k // 8 * 8
        done, rest = both[:top], both[top:]
        row_at = below[top:]
        panel = [jnp.broadcast_to(rest[:, j:j + 1], rest.shape) for j in range(k, k + width)]
        for i in range(width):
            at = k + i - top
            ratio = jnp.where(row_at > k + i, panel[i] * (1.0 / panel[i][at:at + 1]), 0.0)
            for j in range(i + 1, width):
                panel[j] = panel[j] - ratio * panel[j][at:at + 1]
            rest = rest - ratio * rest[at:at + 1]
        both = jnp.concatenate([done, rest], axis=0) if top else rest
        k += width
    return both


def final_kernel(total_size, reduced, wst, pst, out, first_out, second_out, factor_out, first, second, factor, result, out_sem, small_sem):
    terms, depth, rows = wst.shape
    cols = depth // 2
    n_prev = first.shape[0]
    inverse_size = 1.0 / total_size
    root_size = math.sqrt(total_size)
    cross = reduced[:n_prev, :cols] * inverse_size
    self_gram = reduced[:n_prev, cols:] * inverse_size
    basis_gram = reduced[n_prev:, :n_prev] * inverse_size
    turned = cross.T
    once = exact(basis_gram, cross)
    coeff_two = cross - once
    combined = cross + coeff_two
    twice = exact(basis_gram, once)
    back = combined.T
    gram = self_gram - exact(
        jnp.concatenate([turned, back], axis=1),
        jnp.concatenate([combined, coeff_two - once + twice], axis=0))
    first[...] = cross * root_size
    second[...] = coeff_two * root_size
    small_copy = [
        pltpu.make_async_copy(src, dst, small_sem.at[i])
        for i, (src, dst) in enumerate(((first, first_out), (second, second_out), (factor, factor_out)))]
    small_copy[0].start()
    small_copy[1].start()
    row = lax.broadcasted_iota(jnp.int32, (cols, cols), 0)
    lane = lax.broadcasted_iota(jnp.int32, (cols, cols), 1)
    both = jnp.concatenate([gram, jnp.where(row == lane, 1.0, 0.0)], axis=1)
    both = eliminate(both, cols)
    left, right = both[:, :cols], both[:, cols:]
    pivots = jnp.sum(jnp.where(row == lane, left, 0.0), axis=1, keepdims=True)
    scale = 1.0 / jnp.sqrt(pivots)
    inverse = jnp.where(lane <= row, right * scale, 0.0)
    mix = -exact(inverse, back)
    fh, fl = split(inverse)
    dh, dl = split(mix)
    zero_f, zero_d = jnp.zeros_like(fl), jnp.zeros_like(dl)
    weights = jnp.concatenate([
        jnp.concatenate([fh, fh, dh, dh], axis=1),
        jnp.concatenate([fl, zero_f, dl, zero_d], axis=1),
    ], axis=0)
    factor[...] = jnp.where(lane >= row, left * scale, 0.0).T
    small_copy[2].start()
    out_copy = [pltpu.make_async_copy(result.at[t], out.at[t], out_sem.at[t]) for t in range(terms)]
    for t in range(terms):
        both = jnp.dot(weights, jnp.concatenate([wst[t], pst[t]], axis=0), preferred_element_type=F32)
        result[t] = (both[:cols] + both[cols:]).astype(BF)
        out_copy[t].start()
    for copy in small_copy + out_copy:
        copy.wait()


def final(total_size, reduced, wst, pst):
    terms, _, rows = wst.shape
    cols, n_prev = wst.shape[1] // 2, pst.shape[1] // 2
    vmem = pl.BlockSpec(memory_space=pltpu.VMEM)
    hbm = pl.BlockSpec(memory_space=pl.ANY)
    shape = jax.ShapeDtypeStruct
    dma = pltpu.SemaphoreType.DMA
    return pl.pallas_call(
        functools.partial(final_kernel, total_size),
        out_shape=(shape((terms, cols, rows), BF), shape((n_prev, cols), F32), shape((n_prev, cols), F32), shape((cols, cols), F32)),
        in_specs=[vmem] * 3,
        out_specs=(hbm,) * 4,
        scratch_shapes=[
            pltpu.VMEM((n_prev, cols), F32),
            pltpu.VMEM((n_prev, cols), F32),
            pltpu.VMEM((cols, cols), F32),
            pltpu.VMEM((terms, cols, rows), BF),
            dma((terms,)), dma((3,)),
        ],
        compiler_params=pltpu.CompilerParams(vmem_limit_bytes=20 * 1024 * 1024),
    )(reduced, wst, pst)


def body(n_blk, n_col, blocks, offsets, krylov, previous, node_table, node_index, pole_values, scaling):
    terms, cols, rows = krylov.shape
    wst, pst, reduced = expand(
        n_blk, n_col, blocks, offsets, krylov, previous, node_table, node_index, pole_values, scaling)
    return final(rows * n_blk * terms * n_col, reduced, wst, pst)


def solution(mesh):
    in_specs = (
        P("blk", None, None, None),
        P("blk", None),
        P("col", None, "blk"),
        P(None, "col", "blk"),
        P(),
        P("col"),
        P("col"),
        P("col"),
    )
    out_specs = (P("col", None, "blk"), P(), P(), P())
    call = functools.partial(body, mesh.shape["blk"], mesh.shape["col"])
    return jax.shard_map(call, mesh=mesh, in_specs=in_specs, out_specs=out_specs, check_vma=False)
```

```python
import functools
import math

import jax
import jax.numpy as jnp
from jax import lax
from jax.experimental import pallas as pl
from jax.experimental.pallas import tpu as pltpu
from jax.sharding import PartitionSpec as P

REACH = 2
WIDTH = 2 * REACH + 1
GROUP = 2
CHUNK = 256
WINDOW = 3
LAG = 3
SENDS = 4
A_RING = 2 * WINDOW + 1
B_SENDS = 6
D_RING = LAG + 7
BF = jnp.bfloat16
F32 = jnp.float32
NT = (((1,), (1,)), ((), ()))
MESH = pl.DeviceIdType.MESH


def split(x):
    high = x.astype(BF)
    return high, (x - high.astype(F32)).astype(BF)


def dot_nt(a, b):
    return lax.dot_general(a, b, NT, preferred_element_type=F32)


def exact(a, b):
    return jnp.dot(a, b, precision=lax.Precision.HIGHEST, preferred_element_type=F32)


def expand_kernel(
    n_blk, n_col, terms, cols, rows, total_size,
    offsets_in, node_index_in, node_table_in, pole_values_in, scaling_in,
    krylov, blocks, previous,
    wst, pst, reduced,
    offsets, node_index, node_table, pole_values, scaling,
    bufs, carry, band, prev, image, sums, basis_sum,
    a_send, a_recv, b_send, b_recv, c_send, c_recv, d_send, d_recv,
    y_send, y_recv, own_sem, band_sem,
    part, rs_buf, z_buf, ag_buf, red_send, rs_recv, z_recv, ag_recv,
):
    me = lax.axis_index("blk")
    col = lax.axis_index("col")
    core = lax.rem(me, 2)
    chip = lax.div(me, 2)
    par = lax.rem(chip, 2)
    n_chip = n_blk // 2
    n_prev = previous.shape[0]
    partner = (chip + 1 - 2 * par) * 2 + core
    ahead = lax.rem(chip + 2 - 4 * par + n_chip, n_chip) * 2 + core
    sibling = chip * 2 + 1 - core
    per_group = rows // CHUNK
    n_group = terms // GROUP
    n_piece = n_group * per_group

    def remote(src, dst, send, recv, blk, colpos=None):
        return pltpu.make_async_remote_copy(
            src_ref=src, dst_ref=dst, send_sem=send, recv_sem=recv,
            device_id=(blk, col if colpos is None else colpos), device_id_type=MESH)

    def place_of(s):
        if isinstance(s, int):
            return s // per_group, s % per_group
        return lax.div(s, per_group), lax.rem(s, per_group)

    def cut(s):
        if isinstance(s, int) and s >= n_piece - 1:
            start = rows - CHUNK + (s - n_piece + 1) * (CHUNK // 2)
            return pl.ds(terms - GROUP, GROUP), slice(None), pl.ds(start, CHUNK // 2)
        group, k = place_of(s)
        return pl.ds(group * GROUP, GROUP), slice(None), pl.ds(pl.multiple_of(k * CHUNK, CHUNK), CHUNK)

    def ring(s, size):
        return s % size if isinstance(s, int) else lax.rem(s, size)

    def when(test, act):
        if isinstance(test, bool):
            if test:
                act()
        else:
            pl.when(test)(act)

    def a_copy(s):
        return remote(bufs.at[(REACH,) + cut(s)], bufs.at[(4 * par,) + cut(s)], a_send.at[ring(s, SENDS)], a_recv.at[ring(s, A_RING)], partner)

    def b_copy(s):
        return remote(bufs.at[(4 - 4 * par,) + cut(s)], bufs.at[(4 * par,) + cut(s)], b_send.at[ring(s, B_SENDS)], b_recv.at[s], ahead)

    def d_copy(s):
        return remote(bufs.at[(4 - 4 * core,) + cut(s)], bufs.at[(3 - 2 * core,) + cut(s)], d_send.at[ring(s, SENDS)], d_recv.at[ring(s, D_RING)], sibling)

    c_copy = remote(krylov, bufs.at[1 + 2 * core], c_send, c_recv, sibling)
    own_copy = []
    for g in range(n_group):
        some = pl.ds(g * GROUP, GROUP)
        own_copy.append(pltpu.make_async_copy(krylov.at[some], bufs.at[REACH, some], own_sem.at[g]))
    band_copy = [pltpu.make_async_copy(blocks.at[0, c], band.at[c], band_sem.at[c]) for c in range(band.shape[0])]
    prev_copy = pltpu.make_async_copy(previous, prev, red_send.at[5])
    y_copy = remote(krylov.at[terms - 1], carry, y_send, y_recv, me, lax.rem(col + 1, n_col))

    team, depth = part.shape[0], z_buf.shape[0]
    half = team // 2
    place = lax.rem(me, 4)
    layer = lax.div(me, 4)
    pos = place * n_col + col

    def member(j):
        other = lax.rem(pos + j, team)
        return other, layer * 4 + lax.div(other, n_col), lax.rem(other, n_col)

    def peer(j):
        return lax.rem(layer + j, depth) * 4 + place

    def spread(src_of, dst_of, recv, targets):
        return [
            remote(src_of(j), dst_of(j), red_send.at[j - 1], recv.at[j - 1], *target)
            for j, target in targets]

    mates = [(j, member(j)[1:]) for j in range(1, team)]
    peers = [(j, (peer(j), col)) for j in range(1, depth)]
    rs_copy = spread(lambda j: part.at[member(j)[0]], lambda j: rs_buf.at[j - 1], rs_recv, mates)
    z_copy = spread(lambda j: z_buf.at[layer], lambda j: z_buf.at[layer], z_recv, peers)
    ag_copy = spread(lambda j: ag_buf.at[pos], lambda j: ag_buf.at[pos], ag_recv, mates)

    scalar_copy = [
        pltpu.make_async_copy(src, dst, red_send.at[i])
        for i, (src, dst) in enumerate((
            (offsets_in, offsets), (node_index_in, node_index), (node_table_in, node_table),
            (pole_values_in, pole_values), (scaling_in, scaling)))]
    own_copy[0].start()
    for copy in scalar_copy:
        copy.start()
    prev_copy.start()
    for copy in own_copy[1:]:
        copy.start()

    barrier = pltpu.get_barrier_semaphore()
    for j in range(1, team):
        _, blk, at_col = member(j)
        pl.semaphore_signal(barrier, inc=1, device_id=(blk, at_col), device_id_type=MESH)
    for j in range(1, depth):
        pl.semaphore_signal(barrier, inc=1, device_id=(peer(j), col), device_id_type=MESH)
    pl.semaphore_wait(barrier, team + depth - 2)

    own_copy[0].wait()
    lax.fori_loop(0, WINDOW, lambda s, _: (a_copy(s).start(), 0)[1], 0)
    if n_col > 1:
        @pl.when(col < n_col - 1)
        def _():
            y_copy.start()
    c_copy.start()
    for copy in band_copy:
        copy.start()

    @pl.when(col == 0)
    def _():
        carry[...] = jnp.zeros_like(carry)

    lane = 256

    def arrange(t):
        p_at = t * 16

        def step(i, _):
            at = pl.ds(pl.multiple_of(i * lane, lane), lane)
            high, low = split(jnp.swapaxes(prev[p_at:p_at + 16, :, at], 0, 1))
            pst[:, p_at:p_at + 16, at] = high
            pst[:, n_prev + p_at:n_prev + p_at + 16, at] = low
            return 0
        lax.fori_loop(0, rows // lane, step, 0)

    def basis_term(t):
        part = dot_nt(pst[t], pst[t, :n_prev])
        if t == 0:
            basis_sum[...] = part
        else:
            basis_sum[...] += part

    def local_part(t):
        shift = jnp.full((8, 128), node_table[node_index[t]], F32)
        weight = jnp.full((8, 128), scaling[t], F32) / (
            1.0 - shift / jnp.full((8, 128), pole_values[t], F32))
        if t == 0 and n_col > 1:
            @pl.when(col > 0)
            def _():
                y_copy.wait_recv()
        before = carry[...] if t == 0 else bufs[REACH, t - 1]
        image[t * cols:(t + 1) * cols, :] = (
            weight[:1, :1] * before.astype(F32) - shift[:1, :1] * bufs[REACH, t].astype(F32))

    tile = 256
    n_coupling = band.shape[0]

    def selected(r):
        some, _, k_at = cut(r)
        slots = [bufs[j, some, :, k_at].reshape(GROUP * cols, k_at.size) for j in range(WIDTH)]
        picks = []
        for c in range(n_coupling):
            pick = slots[0]
            for j in range(1, WIDTH):
                pick = jnp.where(offsets[0, c] == j - REACH, slots[j], pick)
            picks.append(pick)
        return jnp.concatenate(picks, axis=1)

    def weights_at(at, k_at):
        return jnp.concatenate([band[c, at, k_at] for c in range(n_coupling)], axis=1)

    def compute(r):
        some, _, k_at = cut(r)
        first = some.start * cols
        r_at = pl.ds(first if isinstance(r, int) else pl.multiple_of(first, GROUP * cols), GROUP * cols)
        left = selected(r)

        def step(i, _):
            at = pl.ds(pl.multiple_of(i * tile, tile), tile)
            image[r_at, at] += dot_nt(left, weights_at(at, k_at))
            return 0
        lax.fori_loop(0, rows // tile, step, 0, unroll=UNROLL)

    def finish(t):
        at = pl.ds(t * cols, cols) if isinstance(t, int) else pl.ds(pl.multiple_of(t * cols, cols), cols)
        high, low = split(image[at, :])
        wst[t, :cols] = high
        wst[t, cols:] = low
        sums[...] += dot_nt(jnp.concatenate([pst[t], wst[t]], axis=0), wst[t])

    def forward_a(s):
        a_copy(s).wait_recv()
        when(s >= B_SENDS, lambda: b_copy(s - B_SENDS).wait_send())
        b_copy(s).start()

        @pl.when(par == core)
        def _():
            when(s >= SENDS, lambda: d_copy(s - SENDS).wait_send())
            d_copy(s).start()

    def refill(s):
        when(s >= SENDS, lambda: a_copy(s - SENDS).wait_send())
        a_copy(s).start()

    def forward_b(s):
        b_copy(s).wait_recv()

        @pl.when(par != core)
        def _():
            when(s >= SENDS, lambda: d_copy(s - SENDS).wait_send())
            d_copy(s).start()

    sums[...] = jnp.zeros_like(sums)
    prev_copy.wait()
    for t in range(n_prev // 16):
        arrange(t)
    for copy in scalar_copy + own_copy[1:]:
        copy.wait()
    plan = {}
    for t in range(terms):
        at = t * (LAG + 1) // terms
        plan.setdefault(at, []).append(functools.partial(basis_term, t))
        plan.setdefault(at, []).append(functools.partial(local_part, terms - 1 - t))
    for s in range(LAG + 1):
        forward_a(s)
        refill(s + WINDOW)
        for item in plan.get(s, ()):
            item()
        if s >= LAG:
            forward_b(s - LAG)
    low = basis_sum[n_prev:]
    basis = basis_sum[:n_prev] + low + low.T
    part[half:] = jnp.concatenate([basis, jnp.zeros_like(basis)], axis=1).reshape(half, *part.shape[1:])
    c_copy.wait_recv()
    for copy in band_copy:
        copy.wait()

    last = n_piece - 1

    def main(s, _):
        @pl.when(s < last)
        def _():
            forward_a(s)

        @pl.when(s == last)
        def _():
            forward_a(last)

        @pl.when(s + WINDOW < last)
        def _():
            refill(s + WINDOW)

        @pl.when(s + WINDOW == last)
        def _():
            refill(last)
            refill(last + 1)
        r = s - LAG - 2
        @pl.when(r >= 0)
        def _():
            @pl.when(r < last)
            def _():
                d_copy(r).wait_recv()

            @pl.when(r == last)
            def _():
                d_copy(last).wait_recv()
                d_copy(last + 1).wait_recv()
            compute(r)
        group, k = place_of(r)

        @pl.when((r >= 0) & (k == per_group - 1))
        def _():
            for j in range(GROUP):
                finish(group * GROUP + j)
        @pl.when(s == last)
        def _():
            forward_a(last + 1)

        @pl.when(s < last + LAG)
        def _():
            forward_b(s - LAG)

        @pl.when(s == last + LAG)
        def _():
            forward_b(last)
            forward_b(last + 1)
        return 0
    lax.fori_loop(LAG + 1, n_piece + LAG + 2, main, 0)
    total = sums[:n_prev] + sums[n_prev:2 * n_prev]
    gram = sums[2 * n_prev:2 * n_prev + cols] + sums[2 * n_prev + cols:]
    full = jnp.concatenate([total[:, :cols] + total[:, cols:], gram[:, :cols] + gram[:, cols:]], axis=1)
    part[:half] = full.reshape(half, *part.shape[1:])
    for copy in rs_copy:
        copy.start()
    total = part[pos]
    for j, copy in enumerate(rs_copy):
        copy.wait_recv()
        total = total + rs_buf[j]
    z_buf[layer] = total
    for copy in rs_copy:
        copy.wait_send()
    for copy in z_copy:
        copy.start()
    for s in range(n_piece + 1 - B_SENDS, n_piece + 1):
        if s >= n_piece + 1 - SENDS:
            a_copy(s).wait_send()
        b_copy(s).wait_send()
        if s >= n_piece + 1 - SENDS:
            d_copy(s).wait_send()
    c_copy.wait_send()
    if n_col > 1:
        @pl.when(col < n_col - 1)
        def _():
            y_copy.wait_send()
    for copy in z_copy:
        copy.wait_recv()
    total = z_buf[0]
    for j in range(1, depth):
        total = total + z_buf[j]
    ag_buf[pos] = total
    for copy in z_copy:
        copy.wait_send()
    for copy in ag_copy:
        copy.start()
    for copy in ag_copy:
        copy.wait_recv()
    reduced[...] = ag_buf[...].reshape(reduced.shape)
    for copy in ag_copy:
        copy.wait_send()


UNROLL = 8


def expand(n_blk, n_col, blocks, offsets, krylov, previous, node_table, node_index, pole_values, scaling):
    terms, cols, rows = krylov.shape
    n_prev = previous.shape[0]
    hbm = pl.BlockSpec(memory_space=pl.ANY)
    vmem = pl.BlockSpec(memory_space=pltpu.VMEM)
    dma = pltpu.SemaphoreType.DMA
    team, depth = 4 * n_col, n_blk // 4
    n_group = terms // GROUP
    n_piece = n_group * (rows // CHUNK)
    height = n_prev + cols
    piece = (height // team, 2 * cols)
    return pl.pallas_call(
        functools.partial(expand_kernel, n_blk, n_col, terms, cols, rows, rows * n_blk * terms * n_col),
        out_shape=(
            pltpu.VMEM((terms, 2 * cols, rows), BF),
            pltpu.VMEM((terms, 2 * n_prev, rows), BF),
            pltpu.VMEM((height, 2 * cols), F32),
        ),
        in_specs=[pl.BlockSpec(memory_space=pltpu.HBM)] * 5 + [hbm] * 3,
        out_specs=(vmem,) * 3,
        scratch_shapes=[
            pltpu.SMEM(x.shape, x.dtype) for x in (offsets, node_index, node_table, pole_values, scaling)
        ] + [
            pltpu.VMEM((WIDTH, terms, cols, rows), BF),
            pltpu.VMEM((cols, rows), BF),
            pltpu.VMEM(blocks.shape[1:], BF),
            pltpu.VMEM(previous.shape, F32),
            pltpu.VMEM((terms * cols, rows), F32),
            pltpu.VMEM((2 * n_prev + 2 * cols, 2 * cols), F32),
            pltpu.VMEM((2 * n_prev, n_prev), F32),
        ] + [dma((n,)) for n in (SENDS, A_RING, B_SENDS, n_piece + 1)] + [dma, dma] + [dma((n,)) for n in (SENDS, D_RING)]
        + [dma, dma, dma((n_group,)), dma((blocks.shape[1],))] + [
            pltpu.VMEM((team,) + piece, F32),
            pltpu.VMEM((team - 1,) + piece, F32),
            pltpu.VMEM((depth,) + piece, F32),
            pltpu.VMEM((team,) + piece, F32),
        ] + [dma((n - 1,)) for n in (max(team, depth), team, depth, team)],
        compiler_params=pltpu.CompilerParams(
            collective_id=0, has_side_effects=True, vmem_limit_bytes=58589184),
    )(offsets, node_index, node_table, pole_values, scaling, krylov, blocks, previous)


def eliminate(both, cols):
    below = lax.broadcasted_iota(jnp.int32, (cols, 1), 0)
    k = 0
    while k < cols:
        width = 8 if k < 3 * cols // 4 else 16
        top = k // 8 * 8
        done, rest = both[:top], both[top:]
        row_at = below[top:]
        panel = [jnp.broadcast_to(rest[:, j:j + 1], rest.shape) for j in range(k, k + width)]
        for i in range(width):
            at = k + i - top
            ratio = jnp.where(row_at > k + i, panel[i] * (1.0 / panel[i][at:at + 1]), 0.0)
            for j in range(i + 1, width):
                panel[j] = panel[j] - ratio * panel[j][at:at + 1]
            rest = rest - ratio * rest[at:at + 1]
        both = jnp.concatenate([done, rest], axis=0) if top else rest
        k += width
    return both


def final_kernel(total_size, reduced, wst, pst, out, first_out, second_out, factor_out, first, second, factor, result, out_sem, small_sem):
    terms, depth, rows = wst.shape
    cols = depth // 2
    n_prev = first.shape[0]
    inverse_size = 1.0 / total_size
    root_size = math.sqrt(total_size)
    cross = reduced[:n_prev, :cols] * inverse_size
    self_gram = reduced[:n_prev, cols:] * inverse_size
    basis_gram = reduced[n_prev:, :n_prev] * inverse_size
    turned = cross.T
    once = exact(basis_gram, cross)
    coeff_two = cross - once
    combined = cross + coeff_two
    twice = exact(basis_gram, once)
    back = combined.T
    gram = self_gram - exact(
        jnp.concatenate([turned, back], axis=1),
        jnp.concatenate([combined, coeff_two - once + twice], axis=0))
    first[...] = cross * root_size
    second[...] = coeff_two * root_size
    small_copy = [
        pltpu.make_async_copy(src, dst, small_sem.at[i])
        for i, (src, dst) in enumerate(((first, first_out), (second, second_out), (factor, factor_out)))]
    small_copy[0].start()
    small_copy[1].start()
    row = lax.broadcasted_iota(jnp.int32, (cols, cols), 0)
    lane = lax.broadcasted_iota(jnp.int32, (cols, cols), 1)
    both = jnp.concatenate([gram, jnp.where(row == lane, 1.0, 0.0)], axis=1)
    both = eliminate(both, cols)
    left, right = both[:, :cols], both[:, cols:]
    pivots = jnp.sum(jnp.where(row == lane, left, 0.0), axis=1, keepdims=True)
    scale = 1.0 / jnp.sqrt(pivots)
    inverse = jnp.where(lane <= row, right * scale, 0.0)
    mix = -exact(inverse, back)
    fh, fl = split(inverse)
    dh, dl = split(mix)
    zero_f, zero_d = jnp.zeros_like(fl), jnp.zeros_like(dl)
    weights = jnp.concatenate([
        jnp.concatenate([fh, fh, dh, dh], axis=1),
        jnp.concatenate([fl, zero_f, dl, zero_d], axis=1),
    ], axis=0)
    factor[...] = jnp.where(lane >= row, left * scale, 0.0).T
    small_copy[2].start()
    out_copy = [pltpu.make_async_copy(result.at[t], out.at[t], out_sem.at[t]) for t in range(terms)]
    for t in range(terms):
        both = jnp.dot(weights, jnp.concatenate([wst[t], pst[t]], axis=0), preferred_element_type=F32)
        result[t] = (both[:cols] + both[cols:]).astype(BF)
        out_copy[t].start()
    for copy in small_copy + out_copy:
        copy.wait()


def final(total_size, reduced, wst, pst):
    terms, _, rows = wst.shape
    cols, n_prev = wst.shape[1] // 2, pst.shape[1] // 2
    vmem = pl.BlockSpec(memory_space=pltpu.VMEM)
    hbm = pl.BlockSpec(memory_space=pl.ANY)
    shape = jax.ShapeDtypeStruct
    dma = pltpu.SemaphoreType.DMA
    return pl.pallas_call(
        functools.partial(final_kernel, total_size),
        out_shape=(shape((terms, cols, rows), BF), shape((n_prev, cols), F32), shape((n_prev, cols), F32), shape((cols, cols), F32)),
        in_specs=[vmem] * 3,
        out_specs=(hbm,) * 4,
        scratch_shapes=[
            pltpu.VMEM((n_prev, cols), F32),
            pltpu.VMEM((n_prev, cols), F32),
            pltpu.VMEM((cols, cols), F32),
            pltpu.VMEM((terms, cols, rows), BF),
            dma((terms,)), dma((3,)),
        ],
        compiler_params=pltpu.CompilerParams(vmem_limit_bytes=20 * 1024 * 1024),
    )(reduced, wst, pst)


def body(n_blk, n_col, blocks, offsets, krylov, previous, node_table, node_index, pole_values, scaling):
    terms, cols, rows = krylov.shape
    wst, pst, reduced = expand(
        n_blk, n_col, blocks, offsets, krylov, previous, node_table, node_index, pole_values, scaling)
    return final(rows * n_blk * terms * n_col, reduced, wst, pst)


def solution(mesh):
    in_specs = (
        P("blk", None, None, None),
        P("blk", None),
        P("col", None, "blk"),
        P(None, "col", "blk"),
        P(),
        P("col"),
        P("col"),
        P("col"),
    )
    out_specs = (P("col", None, "blk"), P(), P(), P())
    call = functools.partial(body, mesh.shape["blk"], mesh.shape["col"])
    return jax.shard_map(call, mesh=mesh, in_specs=in_specs, out_specs=out_specs, check_vma=False)
```
